256 devices in a mesh: blk: 16 (over x_lo, y, core), walk: 16 (over x_hi, z).
Axes of the slice: x: 4 (x_hi: 2, x_lo: 2; x = x_hi * 2 + x_lo), y: 4, z: 8, core: 2. Of those that a mesh axis runs over, the one named last changes fastest.
Arguments:
- walkers: bfloat16 [512, 200, 2048], P(('blk', 'walk')), may hold values from -6 to 6
- inv_intersection: bfloat16 [512, 2, 100, 100], P(('blk', 'walk')), may hold values from -0.625 to 0.625
- rotated_chol: bfloat16 [32, 100, 2048], P('blk'), may hold values from -0.013671875 to 0.013671875
- full_chol: bfloat16 [32, 2048, 2048], P('walk', 'blk'), may hold values from -0.125 to 0.125
- field_noise: float32 [32], replicated, may hold values from -4 to 4
Outputs:
- propagated: bfloat16 [512, 200, 2048], P(('blk', 'walk'))
- force_bias: float32 [512, 32], P(('blk', 'walk'))
- bias_shift: float32 [32], replicated
The draws below stay inside these ranges and needn't reach their ends.
All inputs are finite; a program needn't handle non-finite values.
Results may differ from the reference program's by a relative error of at most 0.0065.
Values may be sent and summed in bfloat16 or wider, within the bound.
No kernel may reach another device: no remote copies, remote signals or barrier semaphores. Data moves between devices by JAX's collectives and lax.ppermute only.
A program may use at most 128 MiB of HBM per device.

```python
import jax
import jax.numpy as jnp
from jax import lax

NORB = 2048
NOCC = 100
WALKERS = 512
CHOL = 32


def block_levels(stream_key, shape, split, least, top_value):
    loudness = 1.0
    for position, parts in split:
        draws = jax.random.uniform(jax.random.fold_in(jax.random.fold_in(stream_key, 6), position), (parts,), jnp.float32, least / len(split), top_value / len(split))
        loudness = loudness * jnp.repeat(jnp.exp(draws), shape[position] // parts).reshape((-1,) + (1,) * (len(shape) - 1 - position))
    return loudness


def scatter_about(own_key, extent, scale, reach, cuts=(), dtype=jnp.bfloat16):
    factor_of = block_levels(own_key, extent, cuts, -0.22, 0.18) if cuts else 1.0
    array = jax.random.normal(own_key, extent, jnp.float32) * scale * factor_of
    return jnp.minimum(jnp.maximum(array, -reach), reach).astype(dtype)


def setup_inputs(seed: int = 0) -> dict:
    splits = jax.random.split(jax.random.key(seed), 6)
    return {
        "walkers": scatter_about(splits[0], (WALKERS, 2 * NOCC, NORB), 1.0, 6.0, ((0, 256),)),
        "inv_intersection": scatter_about(splits[1], (WALKERS, 2, NOCC, NOCC), NOCC ** -0.5, 0.625, ((0, 256),)),
        "rotated_chol": scatter_about(splits[2], (CHOL, NOCC, NORB), (NOCC * NORB) ** -0.5, 0.013671875, ((0, 16),)),
        "full_chol": scatter_about(splits[3], (CHOL, NORB, NORB), NORB ** -0.5, 0.125, ((0, 16), (1, 16))),
        "field_noise": scatter_about(splits[4], (CHOL,), 1.0, 4.0, (), jnp.float32),
    }


def reference(walkers, inv_intersection, rotated_chol, full_chol, field_noise):
    spins = walkers.reshape(WALKERS, 2, NOCC, NORB)
    theta = jnp.einsum('wsij,wsjp->wip', inv_intersection.astype(jnp.float32), spins.astype(jnp.float32)).astype(jnp.bfloat16)
    force_bias = jnp.einsum('wip,gip->wg', theta.astype(jnp.float32), rotated_chol.astype(jnp.float32))
    bias_shift = lax.optimization_barrier(jnp.sum(force_bias, axis=0)) / jnp.sqrt(jnp.float32(WALKERS))
    shifted = field_noise - bias_shift
    field = 0.1 * jnp.einsum('g,gij->ij', shifted, full_chol.astype(jnp.float32), precision=lax.Precision.HIGHEST)
    field = field.astype(jnp.bfloat16)
    current = walkers.reshape(WALKERS * 2 * NOCC, NORB)
    total = current.astype(jnp.float32)
    for order in range(1, 5):
        current = (jnp.dot(current, field, preferred_element_type=jnp.float32) / order).astype(jnp.bfloat16)
        total = total + current.astype(jnp.float32)
    propagated = total.astype(jnp.bfloat16).reshape(WALKERS, 2 * NOCC, NORB)
    return (propagated, force_bias, bias_shift)
```

```python
import math

import jax
import jax.numpy as jnp
from jax import lax
from jax.experimental import pallas as pl
from jax.experimental.pallas import tpu as pltpu
from jax.sharding import Mesh
from jax.sharding import PartitionSpec as P

BLK = ("blk_0", "blk_1", "blk_2")
WALK = ("walk_0", "walk_1")
ALL = BLK + WALK
ROWS = 16


def bias_kernel(theta_ref, chol_ref, out_ref):
    walkers, padded, lanes = theta_ref.shape
    vectors = chol_ref.shape[0]
    m, n = walkers * ROWS, vectors * ROWS
    total = jnp.zeros((m, n), jnp.float32)
    for t in range(padded // ROWS):
        a = theta_ref[:, t * ROWS : (t + 1) * ROWS, :].reshape(m, lanes)
        b = chol_ref[:, t * ROWS : (t + 1) * ROWS, :].reshape(n, lanes)
        total = total + lax.dot_general(
            a, b, (((1,), (1,)), ((), ())), preferred_element_type=jnp.float32
        )
    row = lax.broadcasted_iota(jnp.int32, (m, n), 0) % ROWS
    col = lax.broadcasted_iota(jnp.int32, (m, n), 1) % ROWS
    kept = jnp.where(row == col, total, 0.0)
    by_walker = kept.reshape(walkers, ROWS, n).sum(axis=1)
    group = lax.broadcasted_iota(jnp.int32, (n, vectors), 0) // ROWS
    vector = lax.broadcasted_iota(jnp.int32, (n, vectors), 1)
    pick = (group == vector).astype(jnp.float32)
    out_ref[...] = jnp.dot(
        by_walker, pick, preferred_element_type=jnp.float32, precision=lax.Precision.HIGHEST
    )


def partial_bias(theta, chol):
    walkers, vectors = theta.shape[0], chol.shape[0]
    steps = theta.shape[1] // ROWS
    return pl.pallas_call(
        bias_kernel,
        out_shape=jax.ShapeDtypeStruct((walkers, vectors), jnp.float32),
        in_specs=[pl.BlockSpec(memory_space=pltpu.VMEM)] * 2,
        out_specs=pl.BlockSpec(memory_space=pltpu.VMEM),
        cost_estimate=pl.CostEstimate(
            flops=2 * steps * walkers * vectors * ROWS * ROWS * 128,
            bytes_accessed=2 * (theta.size + chol.size),
            transcendentals=0,
        ),
        compiler_params=pltpu.CompilerParams(vmem_limit_bytes=16 * 1024 * 1024),
    )(theta, chol)


def column_blocks(array, count):
    *lead, columns = array.shape
    return jnp.moveaxis(array.reshape(*lead, count, columns // count), -2, 0)


def exchanged(blocks, axes):
    return lax.all_to_all(blocks, axes, split_axis=0, concat_axis=0, tiled=True)


def part(walkers, inv_intersection, rotated_chol, full_chol, field_noise):
    wdev, double_rows, orbitals = walkers.shape
    occupied = double_rows // 2
    n_blk, n_walk = lax.axis_size(BLK), lax.axis_size(WALK)
    n_all = n_blk * n_walk
    padded = -(-occupied // ROWS) * ROWS
    pad = padded - occupied

    width = orbitals // n_blk
    chol = exchanged(column_blocks(rotated_chol, n_blk), BLK)
    chol_all = jnp.pad(chol, ((0, 0), (0, 0), (0, pad), (0, 0))).reshape(-1, padded, width)
    inv = jnp.moveaxis(inv_intersection, 1, 2).reshape(wdev, occupied, double_rows)
    inv = jnp.pad(inv, ((0, 0), (0, pad), (0, 0)))
    theta = jnp.einsum("wij,wjp->wip", inv, walkers, preferred_element_type=jnp.float32)
    theta = theta.astype(jnp.bfloat16)
    theta_all = exchanged(column_blocks(theta, n_blk), BLK)
    theta_all = theta_all.reshape(n_blk * wdev, padded, width)
    partial = partial_bias(theta_all, chol_all)
    vectors = partial.shape[1]

    row = jnp.pad(jnp.sum(partial, axis=0), (0, 128 - vectors))
    rows = exchanged(jnp.broadcast_to(row[None, None], (n_all, 1, 128)), ALL)
    bias_shift = jnp.sum(rows, axis=(0, 1))[:vectors] / math.sqrt(wdev * n_all)
    bias = jnp.sum(exchanged(partial.reshape(n_blk, wdev, vectors), BLK), axis=0)

    shifted = 0.1 * (field_noise - bias_shift)
    own = full_chol.shape[0]
    mine = lax.dynamic_slice_in_dim(shifted, lax.axis_index(WALK) * own, own)
    part_field = jnp.sum(mine[:, None, None] * full_chol.astype(jnp.float32), axis=0)
    part_field = part_field.astype(jnp.bfloat16).reshape(n_walk, -1, orbitals)
    parts = exchanged(part_field, WALK)
    piece = jnp.sum(parts.astype(jnp.float32), axis=0).astype(jnp.bfloat16)
    pieces = exchanged(jnp.broadcast_to(piece[None], (n_walk, *piece.shape)), WALK)
    row_block = pieces.reshape(-1, orbitals)
    field = lax.all_gather(row_block, BLK, axis=0, tiled=True)

    current = walkers.reshape(wdev * double_rows, orbitals)
    total = current.astype(jnp.float32)
    for order in range(1, 5):
        current = (jnp.dot(current, field, preferred_element_type=jnp.float32) / order).astype(
            jnp.bfloat16
        )
        total = total + current.astype(jnp.float32)
    propagated = total.astype(jnp.bfloat16).reshape(wdev, double_rows, orbitals)
    return propagated, bias, bias_shift


def solution(mesh):
    torus = Mesh(mesh.devices.reshape(2, 4, 2, 2, 8), ALL)
    in_specs = (
        P(ALL, None, None),
        P(ALL, None, None, None),
        P(BLK, None, None),
        P(WALK, BLK, None),
        P(),
    )
    out_specs = (P(ALL, None, None), P(ALL, None), P())
    return jax.shard_map(part, mesh=torus, in_specs=in_specs, out_specs=out_specs, check_vma=False)
```

```python
import functools
import math

import jax
import jax.numpy as jnp
from jax import lax
from jax.experimental import pallas as pl
from jax.experimental.pallas import tpu as pltpu
from jax.sharding import Mesh
from jax.sharding import PartitionSpec as P

BLK = ("blk_0", "blk_1", "blk_2")
WALK = ("walk_0", "walk_1")
ALL = BLK + WALK
ROWS = 16
TILE = 256


def theta_kernel(inv_ref, walkers_ref, chol_ref, out_ref):
    blocks, both, padded, width = out_ref.shape
    wdev = walkers_ref.shape[0]
    occupied = chol_ref.shape[1]
    for k in range(blocks):
        columns = slice(k * width, (k + 1) * width)
        for w in range(wdev):
            theta = jnp.dot(
                inv_ref[w], walkers_ref[w, :, columns], preferred_element_type=jnp.float32
            )
            out_ref[k, w] = theta.astype(out_ref.dtype)
        for g in range(both - wdev):
            rows = chol_ref[g, :, columns]
            rest = jnp.zeros((padded - occupied, width), rows.dtype)
            out_ref[k, wdev + g] = jnp.concatenate([rows, rest], axis=0)


def theta_and_chol(inv, walkers, chol, blocks):
    wdev, padded, double_rows = inv.shape
    orbitals = walkers.shape[2]
    shape = (blocks, wdev + chol.shape[0], padded, orbitals // blocks)
    return pl.pallas_call(
        theta_kernel,
        out_shape=jax.ShapeDtypeStruct(shape, jnp.bfloat16),
        in_specs=[pl.BlockSpec(memory_space=pltpu.VMEM)] * 3,
        out_specs=pl.BlockSpec(memory_space=pltpu.VMEM),
        cost_estimate=pl.CostEstimate(
            flops=2 * wdev * padded * double_rows * orbitals,
            bytes_accessed=2 * (walkers.size + chol.size + math.prod(shape)),
            transcendentals=0,
        ),
        compiler_params=pltpu.CompilerParams(vmem_limit_bytes=16 * 1024 * 1024),
    )(inv, walkers, chol)


def bias_kernel(wdev, both_ref, out_ref):
    blocks, both, padded, lanes = both_ref.shape
    vdev = both - wdev
    walkers, vectors = blocks * wdev, blocks * vdev
    m, n = walkers * ROWS, vectors * ROWS
    total = jnp.zeros((m, n), jnp.float32)
    for t in range(padded // ROWS):
        rows = slice(t * ROWS, (t + 1) * ROWS)
        a = both_ref[:, :wdev, rows, :].reshape(m, lanes)
        b = both_ref[:, wdev:, rows, :].reshape(n, lanes)
        total = total + lax.dot_general(
            a, b, (((1,), (1,)), ((), ())), preferred_element_type=jnp.float32
        )
    row = lax.broadcasted_iota(jnp.int32, (m, n), 0) % ROWS
    col = lax.broadcasted_iota(jnp.int32, (m, n), 1) % ROWS
    kept = jnp.where(row == col, total, 0.0)
    by_walker = kept.reshape(walkers, ROWS, n).sum(axis=1)
    group = lax.broadcasted_iota(jnp.int32, (n, vectors), 0) // ROWS
    vector = lax.broadcasted_iota(jnp.int32, (n, vectors), 1)
    pick = (group == vector).astype(jnp.float32)
    out_ref[...] = jnp.dot(
        by_walker, pick, preferred_element_type=jnp.float32, precision=lax.Precision.HIGHEST
    )


def partial_bias(both, wdev):
    blocks, held, padded, lanes = both.shape
    walkers, vectors = blocks * wdev, blocks * (held - wdev)
    return pl.pallas_call(
        functools.partial(bias_kernel, wdev),
        out_shape=jax.ShapeDtypeStruct((walkers, vectors), jnp.float32),
        in_specs=[pl.BlockSpec(memory_space=pltpu.VMEM)],
        out_specs=pl.BlockSpec(memory_space=pltpu.VMEM),
        cost_estimate=pl.CostEstimate(
            flops=2 * walkers * vectors * ROWS * padded * lanes,
            bytes_accessed=2 * both.size,
            transcendentals=0,
        ),
        compiler_params=pltpu.CompilerParams(vmem_limit_bytes=16 * 1024 * 1024),
    )(both)


AROUND = (0, -1, 1, 2)
SECOND = (0, -1, 1, -2, 2)


def places(colour):
    for other in (0, 1):
        for step, far in enumerate(SECOND):
            kept = AROUND if step < 3 else (AROUND[:2] if step == 3 else AROUND[2:])
            yield [((near, far) if colour == 0 else (far, near)) + (other,) for near in kept]


PLACES = [list(places(0)), list(places(1))]


def product_kernel(*refs):
    n_blocks = sum(len(p) for p in PLACES)
    walkers_ref, blocks = refs[0], refs[1 : 1 + n_blocks]
    out_ref, field, current, total, sems = refs[1 + n_blocks :]
    orbitals = field.shape[0]
    height, width = blocks[0].shape[1:]
    x = lax.axis_index("walk_0") * 2 + lax.axis_index("blk_0")
    y, core = lax.axis_index("blk_1"), lax.axis_index("blk_2")
    copies = []
    for colour, operands in enumerate(PLACES):
        for place in operands:
            block = blocks[sum(len(p) for p in PLACES[:colour]) + operands.index(place)]
            for k, (dx, dy, other) in enumerate(place):
                bx, by = (x + dx + 4) % 4, (y + dy + 4) % 4
                bc = core if other == 0 else 1 - core
                row = (((bx % 2) * 4 + by) * 2 + bc) * 2 * height + (bx // 2) * height
                row = pl.multiple_of(row, height)
                copies.append(
                    pltpu.make_async_copy(
                        block.at[k],
                        field.at[pl.ds(row, height), pl.ds(colour * width, width)],
                        sems.at[len(copies)],
                    )
                )
    for copy in copies:
        copy.start()
    for copy in copies:
        copy.wait()
    for order in range(1, 5):
        source = walkers_ref if order == 1 else current.at[order % 2]

        @pl.loop(0, orbitals // TILE)
        def _(n, order=order, source=source):
            columns = pl.ds(pl.multiple_of(n * TILE, TILE), TILE)
            term = jnp.dot(source[...], field[:, columns], preferred_element_type=jnp.float32)
            term = (term / order).astype(jnp.bfloat16)
            before = walkers_ref[:, columns].astype(jnp.float32) if order == 1 else total[:, columns]
            summed = before + term.astype(jnp.float32)
            if order < 4:
                current[(order + 1) % 2, :, columns] = term
                total[:, columns] = summed
            else:
                out_ref[:, columns] = summed.astype(out_ref.dtype)


def propagate(walkers, blocks):
    rows, orbitals = walkers.shape
    copies = sum(len(place) for p in PLACES for place in p)
    return pl.pallas_call(
        product_kernel,
        out_shape=jax.ShapeDtypeStruct((rows, orbitals), walkers.dtype),
        in_specs=[pl.BlockSpec(memory_space=pltpu.VMEM)]
        + [pl.BlockSpec(memory_space=pl.ANY)] * len(blocks),
        out_specs=pl.BlockSpec(memory_space=pltpu.VMEM),
        scratch_shapes=[
            pltpu.VMEM((orbitals, orbitals), jnp.bfloat16),
            pltpu.VMEM((2, rows, orbitals), jnp.bfloat16),
            pltpu.VMEM((rows, orbitals), jnp.float32),
            pltpu.SemaphoreType.DMA((copies,)),
        ],
        cost_estimate=pl.CostEstimate(
            flops=8 * rows * orbitals * orbitals,
            bytes_accessed=2 * (2 * walkers.size + orbitals * orbitals),
            transcendentals=0,
        ),
        compiler_params=pltpu.CompilerParams(vmem_limit_bytes=32 * 1024 * 1024),
    )(walkers, *blocks)


def along(axis):
    if axis == "y":
        names, index = ("blk_1",), lambda v: v % 4
    else:
        names, index = ("blk_0", "walk_0"), lambda v: (v % 2) * 2 + (v % 4) // 2
    return lambda array, steps: lax.ppermute(
        array, names, [(index(v), index(v + steps)) for v in range(4)]
    )


def gathered(own, first, second):
    near = jnp.stack([own] + [first(own, -step) for step in AROUND[1:]])
    below, above = second(near, 1), second(near, -1)
    half = len(AROUND) // 2
    return [near, below, above, second(below[:half], 1), second(above[half:], -1)]


def other_core(array):
    return lax.ppermute(array, "blk_2", [(0, 1), (1, 0)])


def exchanged(blocks, axes):
    return lax.all_to_all(blocks, axes, split_axis=0, concat_axis=0, tiled=True)


def part(walkers, inv_intersection, rotated_chol, full_chol, field_noise):
    wdev, double_rows, orbitals = walkers.shape
    occupied = double_rows // 2
    n_blk, n_walk = lax.axis_size(BLK), lax.axis_size(WALK)
    n_all = n_blk * n_walk
    padded = -(-occupied // ROWS) * ROWS

    inv = jnp.moveaxis(inv_intersection, 1, 2).reshape(wdev, occupied, double_rows)
    inv = jnp.pad(inv, ((0, 0), (0, padded - occupied), (0, 0)))
    both = exchanged(theta_and_chol(inv, walkers, rotated_chol, n_blk), BLK)
    partial = partial_bias(both, wdev)
    vectors = partial.shape[1]

    row = jnp.pad(jnp.sum(partial, axis=0), (0, 128 - vectors))
    rows = exchanged(jnp.broadcast_to(row[None, None], (n_all, 1, 128)), ALL)
    bias_shift = jnp.sum(rows, axis=(0, 1))[:vectors] / math.sqrt(wdev * n_all)
    bias = jnp.sum(exchanged(partial.reshape(n_blk, wdev, vectors), BLK), axis=0)

    shifted = 0.1 * (field_noise - bias_shift)
    own = full_chol.shape[0]
    mine = lax.dynamic_slice_in_dim(shifted, lax.axis_index(WALK) * own, own)
    part_field = jnp.sum(mine[:, None, None] * full_chol.astype(jnp.float32), axis=0)
    part_field = part_field.astype(jnp.bfloat16).reshape(n_walk, -1, orbitals)
    parts = exchanged(part_field, WALK)
    piece = sum(parts[k].astype(jnp.float32) for k in range(n_walk)).astype(jnp.bfloat16)
    n_z = lax.axis_size("walk_1")
    pieces = exchanged(jnp.broadcast_to(piece[None], (n_z, *piece.shape)), "walk_1")
    rows = pieces.reshape(-1, orbitals)
    left, right = rows[:, : orbitals // 2], rows[:, orbitals // 2 :]
    lefts = gathered(left, along("x"), along("y"))
    rights = gathered(right, along("y"), along("x"))
    blocks = []
    for held in (lefts, rights):
        blocks += held + [other_core(array) for array in held]
    propagated = propagate(walkers.reshape(wdev * double_rows, orbitals), blocks)
    propagated = propagated.reshape(walkers.shape)
    return propagated, bias, bias_shift


def solution(mesh):
    torus = Mesh(mesh.devices.reshape(2, 4, 2, 2, 8), ALL)
    in_specs = (
        P(ALL, None, None),
        P(ALL, None, None, None),
        P(BLK, None, None),
        P(WALK, BLK, None),
        P(),
    )
    out_specs = (P(ALL, None, None), P(ALL, None), P())
    return jax.shard_map(part, mesh=torus, in_specs=in_specs, out_specs=out_specs, check_vma=False)
```

```python
import functools
import math

import jax
import jax.numpy as jnp
from jax import lax
from jax.experimental import pallas as pl
from jax.experimental.pallas import tpu as pltpu
from jax.sharding import Mesh
from jax.sharding import PartitionSpec as P

BLK = ("blk_0", "blk_1", "blk_2")
WALK = ("walk_0", "walk_1")
ALL = BLK + WALK
ROWS = 16
TILE = 256
PART = 512


def theta_kernel(inv_ref, walkers_ref, chol_ref, out_ref):
    blocks, both, padded, width = out_ref.shape
    wdev = walkers_ref.shape[0]
    occupied = chol_ref.shape[1]
    for k in range(blocks):
        columns = slice(k * width, (k + 1) * width)
        for w in range(wdev):
            theta = jnp.dot(
                inv_ref[w], walkers_ref[w, :, columns], preferred_element_type=jnp.float32
            )
            out_ref[k, w] = theta.astype(out_ref.dtype)
        for g in range(both - wdev):
            rows = chol_ref[g, :, columns]
            rest = jnp.zeros((padded - occupied, width), rows.dtype)
            out_ref[k, wdev + g] = jnp.concatenate([rows, rest], axis=0)


def theta_and_chol(inv, walkers, chol, blocks):
    wdev, padded, double_rows = inv.shape
    orbitals = walkers.shape[2]
    shape = (blocks, wdev + chol.shape[0], padded, orbitals // blocks)
    return pl.pallas_call(
        theta_kernel,
        out_shape=jax.ShapeDtypeStruct(shape, jnp.bfloat16),
        in_specs=[pl.BlockSpec(memory_space=pltpu.VMEM)] * 3,
        out_specs=pl.BlockSpec(memory_space=pltpu.VMEM),
        cost_estimate=pl.CostEstimate(
            flops=2 * wdev * padded * double_rows * orbitals,
            bytes_accessed=2 * (walkers.size + chol.size + math.prod(shape)),
            transcendentals=0,
        ),
        compiler_params=pltpu.CompilerParams(vmem_limit_bytes=16 * 1024 * 1024),
    )(inv, walkers, chol)


def bias_kernel(wdev, both_ref, out_ref):
    blocks, both, padded, lanes = both_ref.shape
    vdev = both - wdev
    walkers, vectors = blocks * wdev, blocks * vdev
    m, n = walkers * ROWS, vectors * ROWS
    total = jnp.zeros((m, n), jnp.float32)
    for t in range(padded // ROWS):
        rows = slice(t * ROWS, (t + 1) * ROWS)
        a = both_ref[:, :wdev, rows, :].reshape(m, lanes)
        b = both_ref[:, wdev:, rows, :].reshape(n, lanes)
        total = total + lax.dot_general(
            a, b, (((1,), (1,)), ((), ())), preferred_element_type=jnp.float32
        )
    row = lax.broadcasted_iota(jnp.int32, (m, n), 0) % ROWS
    col = lax.broadcasted_iota(jnp.int32, (m, n), 1) % ROWS
    kept = jnp.where(row == col, total, 0.0)
    by_walker = kept.reshape(walkers, ROWS, n).sum(axis=1)
    group = lax.broadcasted_iota(jnp.int32, (n, vectors), 0) // ROWS
    vector = lax.broadcasted_iota(jnp.int32, (n, vectors), 1)
    pick = (group == vector).astype(jnp.float32)
    out_ref[...] = jnp.dot(
        by_walker, pick, preferred_element_type=jnp.float32, precision=lax.Precision.HIGHEST
    )


def partial_bias(both, wdev):
    blocks, held, padded, lanes = both.shape
    walkers, vectors = blocks * wdev, blocks * (held - wdev)
    return pl.pallas_call(
        functools.partial(bias_kernel, wdev),
        out_shape=jax.ShapeDtypeStruct((walkers, vectors), jnp.float32),
        in_specs=[pl.BlockSpec(memory_space=pltpu.VMEM)],
        out_specs=pl.BlockSpec(memory_space=pltpu.VMEM),
        cost_estimate=pl.CostEstimate(
            flops=2 * walkers * vectors * ROWS * padded * lanes,
            bytes_accessed=2 * both.size,
            transcendentals=0,
        ),
        compiler_params=pltpu.CompilerParams(vmem_limit_bytes=16 * 1024 * 1024),
    )(both)


AROUND = (0, -1, 1, 2)
NEAR, NEXT = AROUND[:2], AROUND[2:]
HELD = ((NEAR, 0), (NEXT, 0), (NEAR, -1), (NEXT, -1), (NEAR, 1), (NEXT, 1), (NEAR, 2), (NEXT, 2))


def places(colour):
    for other in (0, 1):
        for kept, far in HELD:
            yield [((near, far) if colour == 0 else (far, near)) + (other,) for near in kept]


PLACES = [list(places(0)), list(places(1))]


def product_kernel(*refs):
    n_blocks = sum(len(p) for p in PLACES)
    walkers_ref, blocks = refs[0], refs[1 : 1 + n_blocks]
    out_ref, field, terms, sems = refs[1 + n_blocks :]
    orbitals = field.shape[0]
    height, width = blocks[0].shape[1:]
    x = lax.axis_index("walk_0") * 2 + lax.axis_index("blk_0")
    y, core = lax.axis_index("blk_1"), lax.axis_index("blk_2")
    parts = [[] for _ in range(2 * width // PART)]
    count = 0
    for first in range(0, width, PART):
        index = 0
        for colour, operands in enumerate(PLACES):
            for place in operands:
                block = blocks[index]
                index += 1
                for k, (dx, dy, other) in enumerate(place):
                    bx, by = (x + dx + 4) % 4, (y + dy + 4) % 4
                    bc = core if other == 0 else 1 - core
                    row = (((bx % 2) * 4 + by) * 2 + bc) * 2 * height + (bx // 2) * height
                    row = pl.multiple_of(row, height)
                    at = colour * width + first
                    copy = pltpu.make_async_copy(
                        block.at[k, :, pl.ds(first, PART)],
                        field.at[pl.ds(row, height), pl.ds(at, PART)],
                        sems.at[count],
                    )
                    count += 1
                    parts[at // PART].append(copy)
    starts = [at for first in range(width // PART) for at in (first, first + width // PART)]
    for at in starts:
        for copy in parts[at]:
            copy.start()

    def term(order, n):
        columns = pl.ds(pl.multiple_of(n * TILE, TILE), TILE)
        source = walkers_ref if order == 1 else terms.at[order - 2]
        product = jnp.dot(source[...], field[:, columns], preferred_element_type=jnp.float32)
        value = (product * (1.0 / order)).astype(jnp.bfloat16)
        if order < 4:
            terms[order - 1, :, columns] = value
        else:
            total = walkers_ref[:, columns].astype(jnp.float32)
            for k in range(3):
                total = total + terms[k, :, columns].astype(jnp.float32)
            out_ref[:, columns] = (total + value.astype(jnp.float32)).astype(out_ref.dtype)

    per_part = PART // TILE
    for at in starts:
        for copy in parts[at]:
            copy.wait()

        @pl.loop(0, 1)
        def _(n, at=at):
            for k in range(per_part):
                term(1, n + at * per_part + k)

    for order in range(2, 5):

        @pl.loop(0, orbitals // TILE // per_part)
        def _(n, order=order):
            for k in range(per_part):
                term(order, n * per_part + k)


def propagate(walkers, blocks):
    rows, orbitals = walkers.shape
    copies = sum(len(place) for p in PLACES for place in p)
    return pl.pallas_call(
        product_kernel,
        out_shape=jax.ShapeDtypeStruct((rows, orbitals), walkers.dtype),
        in_specs=[pl.BlockSpec(memory_space=pltpu.VMEM)]
        + [pl.BlockSpec(memory_space=pl.ANY)] * len(blocks),
        out_specs=pl.BlockSpec(memory_space=pltpu.VMEM),
        scratch_shapes=[
            pltpu.VMEM((orbitals, orbitals), jnp.bfloat16),
            pltpu.VMEM((3, rows, orbitals), jnp.bfloat16),
            pltpu.SemaphoreType.DMA((copies * blocks[0].shape[2] // PART,)),
        ],
        cost_estimate=pl.CostEstimate(
            flops=8 * rows * orbitals * orbitals,
            bytes_accessed=2 * (2 * walkers.size + orbitals * orbitals),
            transcendentals=0,
        ),
        compiler_params=pltpu.CompilerParams(vmem_limit_bytes=32 * 1024 * 1024),
    )(walkers, *blocks)


def along(axis):
    if axis == "y":
        names, index = ("blk_1",), lambda v: v % 4
    else:
        names, index = ("blk_0", "walk_0"), lambda v: (v % 2) * 2 + (v % 4) // 2
    return lambda array, steps: lax.ppermute(
        array, names, [(index(v), index(v + steps)) for v in range(4)]
    )


def gathered(own, first, second):
    came = [own] + [first(own, -step) for step in AROUND[1:]]
    near, next_ = jnp.stack(came[:2]), jnp.stack(came[2:])
    below, above = second(near, 1), second(next_, -1)
    below_next, above_near = second(next_, 1), second(near, -1)
    far = [second(below, 1), second(above, -1)]
    return [near, next_, below, below_next, above_near, above] + far


def other_core(array):
    return lax.ppermute(array, "blk_2", [(0, 1), (1, 0)])


def exchanged(blocks, axes):
    return lax.all_to_all(blocks, axes, split_axis=0, concat_axis=0, tiled=True)


def part(walkers, inv_intersection, rotated_chol, full_chol, field_noise):
    wdev, double_rows, orbitals = walkers.shape
    occupied = double_rows // 2
    n_blk, n_walk = lax.axis_size(BLK), lax.axis_size(WALK)
    n_all = n_blk * n_walk
    padded = -(-occupied // ROWS) * ROWS

    half = lax.axis_index("walk_0")
    rows = full_chol.shape[1] // 2
    kept = lax.dynamic_slice_in_dim(full_chol, half * rows, rows, 1)
    given = lax.dynamic_slice_in_dim(full_chol, (1 - half) * rows, rows, 1)
    came = lax.ppermute(given, "walk_0", [(0, 1), (1, 0)])
    inv = jnp.moveaxis(inv_intersection, 1, 2).reshape(wdev, occupied, double_rows)
    inv = jnp.pad(inv, ((0, 0), (0, padded - occupied), (0, 0)))
    both = theta_and_chol(inv, walkers, rotated_chol, n_blk)
    both = exchanged(both, BLK)
    partial = partial_bias(both, wdev)
    vectors = partial.shape[1]

    summed = jnp.sum(partial, axis=0)
    rows = jnp.concatenate(
        [jnp.broadcast_to(summed, (n_blk, vectors)), partial.reshape(n_blk, wdev * vectors)], axis=1
    )
    rows = jnp.pad(rows, ((0, 0), (0, 128 - rows.shape[1])))
    rows = jnp.broadcast_to(rows[:, None, None], (n_blk, n_walk, 1, 128))
    rows = exchanged(rows.reshape(n_all, 1, 128), ALL)
    rows = rows.reshape(n_blk, n_walk, 128)
    bias_shift = jnp.sum(rows, axis=(0, 1))[:vectors] / math.sqrt(wdev * n_all)
    peers = lax.dynamic_index_in_dim(rows, lax.axis_index(WALK), 1, keepdims=False)
    bias = jnp.sum(peers, axis=0)[vectors : vectors + wdev * vectors].reshape(wdev, vectors)

    shifted = 0.1 * (field_noise - bias_shift)
    own = full_chol.shape[0]
    by_owner = shifted.reshape(2, -1, own)
    mine = lax.dynamic_index_in_dim(by_owner, lax.axis_index("walk_1"), 1, keepdims=False)
    near = lax.dynamic_index_in_dim(mine, half, 0, keepdims=False)
    far = lax.dynamic_index_in_dim(mine, 1 - half, 0, keepdims=False)
    part_field = sum(
        scale[k] * rows[k].astype(jnp.float32)
        for scale, rows in ((near, kept), (far, came))
        for k in range(own)
    )
    n_z = lax.axis_size("walk_1")
    part_field = part_field.astype(jnp.bfloat16).reshape(n_z, -1, orbitals)
    parts = exchanged(part_field, "walk_1")
    piece = sum(parts[k].astype(jnp.float32) for k in range(n_z)).astype(jnp.bfloat16)
    pieces = exchanged(jnp.broadcast_to(piece[None], (n_z, *piece.shape)), "walk_1")
    rows = pieces.reshape(-1, orbitals)
    left, right = rows[:, : orbitals // 2], rows[:, orbitals // 2 :]
    lefts = gathered(left, along("x"), along("y"))
    rights = gathered(right, along("y"), along("x"))
    blocks = []
    for held in (lefts, rights):
        blocks += held + [other_core(array) for array in held]
    propagated = propagate(walkers.reshape(wdev * double_rows, orbitals), blocks)
    propagated = propagated.reshape(walkers.shape)
    return propagated, bias, bias_shift


def solution(mesh):
    torus = Mesh(mesh.devices.reshape(2, 4, 2, 2, 8), ALL)
    in_specs = (
        P(ALL, None, None),
        P(ALL, None, None, None),
        P(BLK, None, None),
        P(WALK, BLK, None),
        P(),
    )
    out_specs = (P(ALL, None, None), P(ALL, None), P())
    return jax.shard_map(part, mesh=torus, in_specs=in_specs, out_specs=out_specs, check_vma=False)
```

```python
import functools
import math

import jax
import jax.numpy as jnp
from jax import lax
from jax.experimental import pallas as pl
from jax.experimental.pallas import tpu as pltpu
from jax.sharding import Mesh
from jax.sharding import PartitionSpec as P

BLK = ("blk_0", "blk_1", "blk_2")
WALK = ("walk_0", "walk_1")
ALL = BLK + WALK
ROWS = 16


def theta_kernel(inv_ref, walkers_ref, chol_ref, out_ref):
    blocks, both, padded, width = out_ref.shape
    wdev = walkers_ref.shape[0]
    occupied = chol_ref.shape[1]
    for k in range(blocks):
        columns = slice(k * width, (k + 1) * width)
        for w in range(wdev):
            theta = jnp.dot(
                inv_ref[w], walkers_ref[w, :, columns], preferred_element_type=jnp.float32
            )
            out_ref[k, w] = theta.astype(out_ref.dtype)
        for g in range(both - wdev):
            rows = chol_ref[g, :, columns]
            rest = jnp.zeros((padded - occupied, width), rows.dtype)
            out_ref[k, wdev + g] = jnp.concatenate([rows, rest], axis=0)


def theta_and_chol(inv, walkers, chol, blocks):
    wdev, padded, double_rows = inv.shape
    orbitals = walkers.shape[2]
    shape = (blocks, wdev + chol.shape[0], padded, orbitals // blocks)
    return pl.pallas_call(
        theta_kernel,
        out_shape=jax.ShapeDtypeStruct(shape, jnp.bfloat16),
        in_specs=[pl.BlockSpec(memory_space=pltpu.VMEM)] * 3,
        out_specs=pl.BlockSpec(memory_space=pltpu.VMEM),
        cost_estimate=pl.CostEstimate(
            flops=2 * wdev * padded * double_rows * orbitals,
            bytes_accessed=2 * (walkers.size + chol.size + math.prod(shape)),
            transcendentals=0,
        ),
        compiler_params=pltpu.CompilerParams(vmem_limit_bytes=16 * 1024 * 1024),
    )(inv, walkers, chol)


def bias_kernel(wdev, both_ref, out_ref):
    blocks, both, padded, lanes = both_ref.shape
    vdev = both - wdev
    walkers, vectors = blocks * wdev, blocks * vdev
    m, n = walkers * ROWS, vectors * ROWS
    total = jnp.zeros((m, n), jnp.float32)
    for t in range(padded // ROWS):
        rows = slice(t * ROWS, (t + 1) * ROWS)
        a = both_ref[:, :wdev, rows, :].reshape(m, lanes)
        b = both_ref[:, wdev:, rows, :].reshape(n, lanes)
        total = total + lax.dot_general(
            a, b, (((1,), (1,)), ((), ())), preferred_element_type=jnp.float32
        )
    row = lax.broadcasted_iota(jnp.int32, (m, n), 0) % ROWS
    col = lax.broadcasted_iota(jnp.int32, (m, n), 1) % ROWS
    kept = jnp.where(row == col, total, 0.0)
    by_walker = kept.reshape(walkers, ROWS, n).sum(axis=1)
    group = lax.broadcasted_iota(jnp.int32, (n, vectors), 0) // ROWS
    vector = lax.broadcasted_iota(jnp.int32, (n, vectors), 1)
    pick = (group == vector).astype(jnp.float32)
    out_ref[...] = jnp.dot(
        by_walker, pick, preferred_element_type=jnp.float32, precision=lax.Precision.HIGHEST
    )


def partial_bias(both, wdev):
    blocks, held, padded, lanes = both.shape
    walkers, vectors = blocks * wdev, blocks * (held - wdev)
    return pl.pallas_call(
        functools.partial(bias_kernel, wdev),
        out_shape=jax.ShapeDtypeStruct((walkers, vectors), jnp.float32),
        in_specs=[pl.BlockSpec(memory_space=pltpu.VMEM)],
        out_specs=pl.BlockSpec(memory_space=pltpu.VMEM),
        cost_estimate=pl.CostEstimate(
            flops=2 * walkers * vectors * ROWS * padded * lanes,
            bytes_accessed=2 * both.size,
            transcendentals=0,
        ),
        compiler_params=pltpu.CompilerParams(vmem_limit_bytes=16 * 1024 * 1024),
    )(both)


AROUND = (0, -1, 1, 2)
NEAR, NEXT = AROUND[:2], AROUND[2:]
HELD = ((NEAR, 0), (NEXT, 0), (NEAR, -1), (NEXT, -1), (NEAR, 1), (NEXT, 1), (NEAR, 2), (NEXT, 2))


def assembly_kernel(*refs):
    blocks, out_ref, sems = refs[: 2 * len(HELD)], refs[2 * len(HELD)], refs[2 * len(HELD) + 1]
    height, width = blocks[0].shape[2:]
    x = lax.axis_index("walk_0") * 2 + lax.axis_index("blk_0")
    y, core = lax.axis_index("blk_1"), lax.axis_index("blk_2")
    copies = []
    for other in (0, 1):
        colour = core if other == 0 else 1 - core
        for array, (kept, far) in enumerate(HELD):
            for k, near in enumerate(kept):
                dx = near + colour * (far - near)
                dy = far + colour * (near - far)
                bx, by = (x + dx + 4) % 4, (y + dy + 4) % 4
                for side in (0, 1):
                    bc = colour if side == 0 else 1 - colour
                    row = (((bx % 2) * 4 + by) * 2 + bc) * 2 * height + (bx // 2) * height
                    row = pl.multiple_of(row, height)
                    column = pl.multiple_of(colour * width, width)
                    copy = pltpu.make_async_copy(
                        blocks[other * len(HELD) + array].at[k, side],
                        out_ref.at[pl.ds(row, height), pl.ds(column, width)],
                        sems.at[len(copies)],
                    )
                    copy.start()
                    copies.append(copy)
    for copy in copies:
        copy.wait()


def assembled(blocks, orbitals):
    return pl.pallas_call(
        assembly_kernel,
        out_shape=jax.ShapeDtypeStruct((orbitals, orbitals), jnp.bfloat16),
        in_specs=[pl.BlockSpec(memory_space=pl.ANY)] * len(blocks),
        out_specs=pl.BlockSpec(memory_space=pltpu.VMEM),
        scratch_shapes=[pltpu.SemaphoreType.DMA((4 * len(blocks),))],
        cost_estimate=pl.CostEstimate(
            flops=orbitals * orbitals, bytes_accessed=4 * orbitals * orbitals, transcendentals=0
        ),
        compiler_params=pltpu.CompilerParams(vmem_limit_bytes=16 * 1024 * 1024),
    )(*blocks)


CHIP = ("blk_0", "blk_1", "blk_2", "walk_0")


def stepped(array, first, steps):
    def device(x, y, core):
        return (((x % 2) * 4 + y % 4) * 2 + core) * 2 + x % 4 // 2

    pairs = []
    for x in range(4):
        for y in range(4):
            for core in (0, 1):
                along_x = first == (core == 0)
                to = (x + steps, y) if along_x else (x, y + steps)
                pairs.append((device(x, y, core), device(*to, core)))
    return lax.ppermute(array, CHIP, pairs)


def other_core(array):
    return lax.ppermute(array, "blk_2", [(0, 1), (1, 0)])


def gathered(rows, core):
    width = rows.shape[1] // 2
    own = lax.dynamic_slice_in_dim(rows, core * width, width, 1, allow_negative_indices=False)
    given = lax.dynamic_slice_in_dim(rows, (1 - core) * width, width, 1, allow_negative_indices=False)
    own = jnp.stack([own, other_core(given)])
    came = [own] + [stepped(own, True, -step) for step in AROUND[1:]]
    near, next_ = jnp.stack(came[:2]), jnp.stack(came[2:])
    below, above = stepped(near, False, 1), stepped(next_, False, -1)
    below_next, above_near = stepped(next_, False, 1), stepped(near, False, -1)
    far = [stepped(below, False, 1), stepped(above, False, -1)]
    held = [near, next_, below, below_next, above_near, above] + far
    return held + [other_core(array) for array in held]


def copy_kernel(in_ref, out_ref):
    out_ref[...] = in_ref[...]


def copied(array):
    return pl.pallas_call(
        copy_kernel,
        out_shape=jax.ShapeDtypeStruct(array.shape, array.dtype),
        in_specs=[pl.BlockSpec(memory_space=pltpu.VMEM)],
        out_specs=pl.BlockSpec(memory_space=pltpu.VMEM),
        cost_estimate=pl.CostEstimate(
            flops=array.size, bytes_accessed=4 * array.size, transcendentals=0
        ),
        compiler_params=pltpu.CompilerParams(vmem_limit_bytes=4 * 1024 * 1024),
    )(array)


def at(array, index, dim):
    return lax.dynamic_index_in_dim(array, index, dim, keepdims=False, allow_negative_indices=False)


def exchanged(blocks, axes):
    return lax.all_to_all(blocks, axes, split_axis=0, concat_axis=0, tiled=True)


def part(walkers, inv_intersection, rotated_chol, full_chol, field_noise):
    wdev, double_rows, orbitals = walkers.shape
    occupied = double_rows // 2
    n_blk, n_walk = lax.axis_size(BLK), lax.axis_size(WALK)
    n_all = n_blk * n_walk
    padded = -(-occupied // ROWS) * ROWS

    inv = jnp.moveaxis(inv_intersection, 1, 2).reshape(wdev, occupied, double_rows)
    inv = jnp.pad(inv, ((0, 0), (0, padded - occupied), (0, 0)))
    both = theta_and_chol(inv, walkers, rotated_chol, n_blk)
    both = exchanged(both, BLK)
    own = full_chol.shape[0]
    n_z = lax.axis_size("walk_1")
    half, at_z = lax.axis_index("walk_0"), lax.axis_index("walk_1")
    raw = full_chol.reshape(own, 2, n_z, -1, orbitals)

    def for_z(step):
        return at(raw, lax.rem(at_z + step, n_z), 2)

    slices = [for_z(step) for step in range(n_z)]
    raws = [copied(slices[0])]
    for step, rows in enumerate(slices[1:], 1):
        pairs = [(k, (k + step) % n_z) for k in range(n_z)]
        raws.append(lax.ppermute(rows, "walk_1", pairs))
    partial = partial_bias(both, wdev)
    vectors = partial.shape[1]

    summed = jnp.sum(partial, axis=0)
    rows = jnp.concatenate(
        [jnp.broadcast_to(summed, (n_blk, vectors)), partial.reshape(n_blk, wdev * vectors)], axis=1
    )
    rows = jnp.pad(rows, ((0, 0), (0, 128 - rows.shape[1])))
    rows = jnp.broadcast_to(rows[:, None, None], (n_blk, n_walk, 1, 128))
    core = lax.axis_index("blk_2")
    rows, half, at_z, core = lax.optimization_barrier((rows, half, at_z, core))
    rows = exchanged(rows.reshape(n_all, 1, 128), ALL)
    rows, half, at_z, core = lax.optimization_barrier((rows, half, at_z, core))
    rows = rows.reshape(n_blk, n_walk, 128)
    bias_shift = jnp.sum(rows, axis=(0, 1))[:vectors] / math.sqrt(wdev * n_all)
    peers = at(rows, half * n_z + at_z, 1)
    bias = jnp.sum(peers, axis=0)[vectors : vectors + wdev * vectors].reshape(wdev, vectors)

    shifted = 0.1 * (field_noise - bias_shift)
    entry = lax.broadcasted_iota(jnp.int32, (n_z * own, vectors), 0)
    vector = lax.broadcasted_iota(jnp.int32, (n_z * own, vectors), 1)
    source = at_z - entry // own
    source = jnp.where(source < 0, source + n_z, source)
    wanted = (half * n_z + source) * own + entry % own
    scale = jnp.sum(jnp.where(vector == wanted, shifted[None, :], 0.0), axis=1)
    part_field = sum(
        scale[step * own + k] * raws[step][k].astype(jnp.float32)
        for step in range(n_z)
        for k in range(own)
    )
    kept = at(part_field, half, 0)
    given = at(part_field, 1 - half, 0)
    came = lax.ppermute(given, "walk_0", [(0, 1), (1, 0)])
    piece = (kept + came).astype(jnp.bfloat16)
    pieces = exchanged(jnp.broadcast_to(piece[None], (n_z, *piece.shape)), "walk_1")
    field = assembled(gathered(pieces.reshape(-1, orbitals), core), orbitals)
    current = walkers.reshape(wdev * double_rows, orbitals)
    total = current.astype(jnp.float32)
    for order in range(1, 5):
        current = (jnp.dot(current, field, preferred_element_type=jnp.float32) / order).astype(
            jnp.bfloat16
        )
        total = total + current.astype(jnp.float32)
    propagated = total.astype(jnp.bfloat16).reshape(walkers.shape)
    return propagated, bias, bias_shift


def solution(mesh):
    torus = Mesh(mesh.devices.reshape(2, 4, 2, 2, 8), ALL)
    in_specs = (
        P(ALL, None, None),
        P(ALL, None, None, None),
        P(BLK, None, None),
        P(WALK, BLK, None),
        P(),
    )
    out_specs = (P(ALL, None, None), P(ALL, None), P())
    return jax.shard_map(part, mesh=torus, in_specs=in_specs, out_specs=out_specs, check_vma=False)
```

```python
import functools
import math

import jax
import jax.numpy as jnp
from jax import lax
from jax.experimental import pallas as pl
from jax.experimental.pallas import tpu as pltpu
from jax.sharding import Mesh
from jax.sharding import PartitionSpec as P

BLK = ("blk_0", "blk_1", "blk_2")
WALK = ("walk_0", "walk_1")
ALL = BLK + WALK
ROWS = 16


def theta_kernel(inv_ref, walkers_ref, chol_ref, out_ref):
    blocks, both, padded, width = out_ref.shape
    wdev = walkers_ref.shape[0]
    for k in range(blocks):
        columns = slice(k * width, (k + 1) * width)
        for w in range(wdev):
            theta = jnp.dot(
                inv_ref[w], walkers_ref[w, :, columns], preferred_element_type=jnp.float32
            )
            out_ref[k, w] = theta.astype(out_ref.dtype)
        for g in range(both - wdev):
            rows = chol_ref[g, :, columns]
            rest = jnp.zeros((padded - rows.shape[0], width), rows.dtype)
            out_ref[k, wdev + g] = jnp.concatenate([rows, rest], axis=0)


def theta_and_chol(inv, walkers, chol, blocks):
    wdev, padded, double_rows = inv.shape
    orbitals = walkers.shape[2]
    shape = (blocks, wdev + chol.shape[0], padded, orbitals // blocks)
    return pl.pallas_call(
        theta_kernel,
        out_shape=jax.ShapeDtypeStruct(shape, jnp.bfloat16),
        in_specs=[pl.BlockSpec(memory_space=pltpu.VMEM)] * 3,
        out_specs=pl.BlockSpec(memory_space=pltpu.VMEM),
        cost_estimate=pl.CostEstimate(
            flops=2 * wdev * padded * double_rows * orbitals,
            bytes_accessed=2 * (walkers.size + chol.size + math.prod(shape)),
            transcendentals=0,
        ),
        compiler_params=pltpu.CompilerParams(vmem_limit_bytes=16 * 1024 * 1024),
    )(inv, walkers, chol)


def bias_kernel(wdev, both_ref, out_ref):
    blocks, both, occupied, lanes = both_ref.shape
    vdev = both - wdev
    walkers, vectors = blocks * wdev, blocks * vdev
    m, n = walkers * ROWS, vectors * ROWS
    total = jnp.zeros((m, n), jnp.float32)
    for first in range(0, occupied, ROWS):
        rows = slice(first, min(first + ROWS, occupied))
        a, b = both_ref[:, :wdev, rows, :], both_ref[:, wdev:, rows, :]
        if first + ROWS > occupied:
            rest = ((0, 0), (0, 0), (0, first + ROWS - occupied), (0, 0))
            a, b = jnp.pad(a, rest), jnp.pad(b, rest)
        a, b = a.reshape(m, lanes), b.reshape(n, lanes)
        total = total + lax.dot_general(
            a, b, (((1,), (1,)), ((), ())), preferred_element_type=jnp.float32
        )
    row = lax.broadcasted_iota(jnp.int32, (m, n), 0) % ROWS
    col = lax.broadcasted_iota(jnp.int32, (m, n), 1) % ROWS
    kept = jnp.where(row == col, total, 0.0)
    by_walker = kept.reshape(walkers, ROWS, n).sum(axis=1)
    group = lax.broadcasted_iota(jnp.int32, (n, vectors), 0) // ROWS
    vector = lax.broadcasted_iota(jnp.int32, (n, vectors), 1)
    pick = (group == vector).astype(jnp.float32)
    out_ref[...] = jnp.dot(
        by_walker, pick, preferred_element_type=jnp.float32, precision=lax.Precision.HIGHEST
    )


def partial_bias(both, wdev):
    blocks, held, occupied, lanes = both.shape
    walkers, vectors = blocks * wdev, blocks * (held - wdev)
    return pl.pallas_call(
        functools.partial(bias_kernel, wdev),
        out_shape=jax.ShapeDtypeStruct((walkers, vectors), jnp.float32),
        in_specs=[pl.BlockSpec(memory_space=pltpu.VMEM)],
        out_specs=pl.BlockSpec(memory_space=pltpu.VMEM),
        cost_estimate=pl.CostEstimate(
            flops=2 * walkers * vectors * ROWS * occupied * lanes,
            bytes_accessed=2 * both.size,
            transcendentals=0,
        ),
        compiler_params=pltpu.CompilerParams(vmem_limit_bytes=16 * 1024 * 1024),
    )(both)


AROUND = (0, -1, 1, 2)
NEAR, NEXT = AROUND[:2], AROUND[2:]
HELD = ((NEAR, 0), (NEXT, 0), (NEAR, -1), (NEXT, -1), (NEAR, 1), (NEXT, 1), (NEAR, 2), (NEXT, 2))


def assembly_kernel(*refs):
    blocks, out_ref, sems = refs[: 2 * len(HELD)], refs[2 * len(HELD)], refs[2 * len(HELD) + 1]
    height, width = blocks[0].shape[2:]
    x = lax.axis_index("walk_0") * 2 + lax.axis_index("blk_0")
    y, core = lax.axis_index("blk_1"), lax.axis_index("blk_2")
    copies = []
    for other in (0, 1):
        colour = core if other == 0 else 1 - core
        for array, (kept, far) in enumerate(HELD):
            for k, near in enumerate(kept):
                dx = near + colour * (far - near)
                dy = far + colour * (near - far)
                bx, by = (x + dx + 4) % 4, (y + dy + 4) % 4
                for side in (0, 1):
                    bc = colour if side == 0 else 1 - colour
                    row = (((bx % 2) * 4 + by) * 2 + bc) * 2 * height + (bx // 2) * height
                    row = pl.multiple_of(row, height)
                    column = pl.multiple_of(colour * width, width)
                    copy = pltpu.make_async_copy(
                        blocks[other * len(HELD) + array].at[k, side],
                        out_ref.at[pl.ds(row, height), pl.ds(column, width)],
                        sems.at[len(copies)],
                    )
                    copy.start()
                    copies.append(copy)
    for copy in copies:
        copy.wait()


def assembled(blocks, orbitals):
    return pl.pallas_call(
        assembly_kernel,
        out_shape=jax.ShapeDtypeStruct((orbitals, orbitals), jnp.bfloat16),
        in_specs=[pl.BlockSpec(memory_space=pl.ANY)] * len(blocks),
        out_specs=pl.BlockSpec(memory_space=pltpu.VMEM),
        scratch_shapes=[pltpu.SemaphoreType.DMA((4 * len(blocks),))],
        cost_estimate=pl.CostEstimate(
            flops=orbitals * orbitals, bytes_accessed=4 * orbitals * orbitals, transcendentals=0
        ),
        compiler_params=pltpu.CompilerParams(vmem_limit_bytes=16 * 1024 * 1024),
    )(*blocks)


CHIP = ("blk_0", "blk_1", "blk_2", "walk_0")


def stepped(array, first, steps):
    def device(x, y, core):
        return (((x % 2) * 4 + y % 4) * 2 + core) * 2 + x % 4 // 2

    pairs = []
    for x in range(4):
        for y in range(4):
            for core in (0, 1):
                along_x = first == (core == 0)
                to = (x + steps, y) if along_x else (x, y + steps)
                pairs.append((device(x, y, core), device(*to, core)))
    return lax.ppermute(array, CHIP, pairs)


def other_core(array):
    return lax.ppermute(array, "blk_2", [(0, 1), (1, 0)])


def gathered(rows, core):
    width = rows.shape[1] // 2
    own = lax.dynamic_slice_in_dim(rows, core * width, width, 1, allow_negative_indices=False)
    given = lax.dynamic_slice_in_dim(rows, (1 - core) * width, width, 1, allow_negative_indices=False)
    own = jnp.stack([own, other_core(given)])
    came = [own] + [stepped(own, True, -step) for step in AROUND[1:3]]
    came.append(stepped(own, True, AROUND[3]))
    near = jnp.stack(came[:2])
    below, above_near = stepped(near, False, 1), stepped(near, False, -1)
    next_ = jnp.stack(came[2:])
    above, below_next = stepped(next_, False, -1), stepped(next_, False, 1)
    far = [stepped(below, False, 1)]
    far.append(stepped(above, False, -1))
    held = [near, next_, below, below_next, above_near, above] + far
    return held + [other_core(array) for array in held]


def copy_kernel(in_ref, out_ref):
    out_ref[...] = in_ref[...]


def copied(array):
    return pl.pallas_call(
        copy_kernel,
        out_shape=jax.ShapeDtypeStruct(array.shape, array.dtype),
        in_specs=[pl.BlockSpec(memory_space=pltpu.VMEM)],
        out_specs=pl.BlockSpec(memory_space=pltpu.VMEM),
        cost_estimate=pl.CostEstimate(
            flops=array.size, bytes_accessed=4 * array.size, transcendentals=0
        ),
        compiler_params=pltpu.CompilerParams(vmem_limit_bytes=4 * 1024 * 1024),
    )(array)


def sum_kernel(scale_ref, *refs):
    raws, out_ref = refs[:-1], refs[-1]
    own, halves = raws[0].shape[:2]
    for h in range(halves):
        total = None
        for step, raw in enumerate(raws):
            for k in range(own):
                value = scale_ref[step * own + k] * raw[k, h].astype(jnp.float32)
                total = value if total is None else total + value
        out_ref[h] = total


def scaled_sum(scale, raws):
    own, *shape = raws[0].shape
    size = own * math.prod(shape) * len(raws)
    return pl.pallas_call(
        sum_kernel,
        out_shape=jax.ShapeDtypeStruct(tuple(shape), jnp.float32),
        in_specs=[pl.BlockSpec(memory_space=pltpu.SMEM)]
        + [pl.BlockSpec(memory_space=pltpu.VMEM)] * len(raws),
        out_specs=pl.BlockSpec(memory_space=pltpu.VMEM),
        cost_estimate=pl.CostEstimate(flops=2 * size, bytes_accessed=2 * size, transcendentals=0),
        compiler_params=pltpu.CompilerParams(vmem_limit_bytes=8 * 1024 * 1024),
    )(scale, *raws)


def at(array, index, dim):
    return lax.dynamic_index_in_dim(array, index, dim, keepdims=False, allow_negative_indices=False)


def exchanged(blocks, axes):
    return lax.all_to_all(blocks, axes, split_axis=0, concat_axis=0, tiled=True)


def part(walkers, inv_intersection, rotated_chol, full_chol, field_noise):
    wdev, double_rows, orbitals = walkers.shape
    occupied = double_rows // 2
    n_blk, n_walk = lax.axis_size(BLK), lax.axis_size(WALK)
    n_all = n_blk * n_walk

    inv = jnp.moveaxis(inv_intersection, 1, 2).reshape(wdev, occupied, double_rows)
    inv = jnp.pad(inv, ((0, 0), (0, -occupied % 8), (0, 0)))
    both = theta_and_chol(inv, walkers, rotated_chol, n_blk)
    both = exchanged(both, BLK)
    own = full_chol.shape[0]
    n_z = lax.axis_size("walk_1")
    half, at_z = lax.axis_index("walk_0"), lax.axis_index("walk_1")
    raw = full_chol.reshape(own, 2, n_z, -1, orbitals)

    def for_z(step):
        return at(raw, lax.rem(at_z + step, n_z), 2)

    slices = [for_z(step) for step in range(n_z)]
    raws = [copied(slices[0])]
    for step, rows in enumerate(slices[1:], 1):
        pairs = [(k, (k + step) % n_z) for k in range(n_z)]
        raws.append(lax.ppermute(rows, "walk_1", pairs))
    partial = partial_bias(both, wdev)
    vectors = partial.shape[1]

    summed = jnp.sum(partial, axis=0)
    rows = jnp.concatenate(
        [jnp.broadcast_to(summed, (n_blk, vectors)), partial.reshape(n_blk, wdev * vectors)], axis=1
    )
    rows = jnp.pad(rows, ((0, 0), (0, 128 - rows.shape[1])))
    rows = jnp.broadcast_to(rows[:, None, None], (n_blk, n_walk, 1, 128))
    core = lax.axis_index("blk_2")
    entry = lax.broadcasted_iota(jnp.int32, (n_z * own, vectors), 0)
    vector = lax.broadcasted_iota(jnp.int32, (n_z * own, vectors), 1)
    source = at_z - entry // own
    source = jnp.where(source < 0, source + n_z, source)
    wanted = (half * n_z + source) * own + entry % own
    ids = (half, at_z, core, vector == wanted)
    rows, (half, at_z, core, picked) = lax.optimization_barrier((rows, ids))
    rows = exchanged(rows.reshape(n_all, 1, 128), ALL)
    ids = (half, at_z, core, picked)
    rows, (half, at_z, core, picked) = lax.optimization_barrier((rows, ids))
    rows = rows.reshape(n_blk, n_walk, 128)
    bias_shift = jnp.sum(rows, axis=(0, 1))[:vectors] / math.sqrt(wdev * n_all)
    peers = at(rows, half * n_z + at_z, 1)
    bias = jnp.sum(peers, axis=0)[vectors : vectors + wdev * vectors].reshape(wdev, vectors)

    shifted = 0.1 * (field_noise - bias_shift)
    scale = jnp.sum(jnp.where(picked, shifted[None, :], 0.0), axis=1)
    part_field = scaled_sum(scale, raws)
    kept = at(part_field, half, 0)
    given = at(part_field, 1 - half, 0)
    came = lax.ppermute(given, "walk_0", [(0, 1), (1, 0)])
    piece = (kept + came).astype(jnp.bfloat16)
    pieces = exchanged(jnp.broadcast_to(piece[None], (n_z, *piece.shape)), "walk_1")
    field = assembled(gathered(pieces.reshape(-1, orbitals), core), orbitals)
    current = walkers.reshape(wdev * double_rows, orbitals)
    total = current.astype(jnp.float32)
    for order in range(1, 5):
        current = (jnp.dot(current, field, preferred_element_type=jnp.float32) / order).astype(
            jnp.bfloat16
        )
        total = total + current.astype(jnp.float32)
    propagated = total.astype(jnp.bfloat16).reshape(walkers.shape)
    return propagated, bias, bias_shift


def solution(mesh):
    torus = Mesh(mesh.devices.reshape(2, 4, 2, 2, 8), ALL)
    in_specs = (
        P(ALL, None, None),
        P(ALL, None, None, None),
        P(BLK, None, None),
        P(WALK, BLK, None),
        P(),
    )
    out_specs = (P(ALL, None, None), P(ALL, None), P())
    return jax.shard_map(part, mesh=torus, in_specs=in_specs, out_specs=out_specs, check_vma=False)
```

```python
import functools
import math

import jax
import jax.numpy as jnp
from jax import lax
from jax.experimental import pallas as pl
from jax.experimental.pallas import tpu as pltpu
from jax.sharding import Mesh
from jax.sharding import PartitionSpec as P

BLK = ("blk_0", "blk_1", "blk_2")
WALK = ("walk_0", "walk_1")
ALL = BLK + WALK
ROWS = 16


def theta_kernel(inv_ref, walkers_ref, chol_ref, out_ref):
    blocks, both, padded, width = out_ref.shape
    wdev = walkers_ref.shape[0]
    for k in range(blocks):
        columns = slice(k * width, (k + 1) * width)
        for w in range(wdev):
            theta = jnp.dot(
                inv_ref[w], walkers_ref[w, :, columns], preferred_element_type=jnp.float32
            )
            out_ref[k, w] = theta.astype(out_ref.dtype)
        for g in range(both - wdev):
            rows = chol_ref[g, :, columns]
            rest = jnp.zeros((padded - rows.shape[0], width), rows.dtype)
            out_ref[k, wdev + g] = jnp.concatenate([rows, rest], axis=0)


def theta_and_chol(inv, walkers, chol, blocks):
    wdev, padded, double_rows = inv.shape
    orbitals = walkers.shape[2]
    shape = (blocks, wdev + chol.shape[0], padded, orbitals // blocks)
    return pl.pallas_call(
        theta_kernel,
        out_shape=jax.ShapeDtypeStruct(shape, jnp.bfloat16),
        in_specs=[pl.BlockSpec(memory_space=pltpu.VMEM)] * 3,
        out_specs=pl.BlockSpec(memory_space=pltpu.VMEM),
        cost_estimate=pl.CostEstimate(
            flops=2 * wdev * padded * double_rows * orbitals,
            bytes_accessed=2 * (walkers.size + chol.size + math.prod(shape)),
            transcendentals=0,
        ),
        compiler_params=pltpu.CompilerParams(vmem_limit_bytes=16 * 1024 * 1024),
    )(inv, walkers, chol)


def bias_kernel(wdev, both_ref, out_ref):
    blocks, both, occupied, lanes = both_ref.shape
    vdev = both - wdev
    walkers, vectors = blocks * wdev, blocks * vdev
    m, n = walkers * ROWS, vectors * ROWS
    total = jnp.zeros((m, n), jnp.float32)
    for first in range(0, occupied, ROWS):
        rows = slice(first, min(first + ROWS, occupied))
        a, b = both_ref[:, :wdev, rows, :], both_ref[:, wdev:, rows, :]
        if first + ROWS > occupied:
            rest = ((0, 0), (0, 0), (0, first + ROWS - occupied), (0, 0))
            a, b = jnp.pad(a, rest), jnp.pad(b, rest)
        a, b = a.reshape(m, lanes), b.reshape(n, lanes)
        total = total + lax.dot_general(
            a, b, (((1,), (1,)), ((), ())), preferred_element_type=jnp.float32
        )
    row = lax.broadcasted_iota(jnp.int32, (m, n), 0) % ROWS
    col = lax.broadcasted_iota(jnp.int32, (m, n), 1) % ROWS
    kept = jnp.where(row == col, total, 0.0)
    by_walker = kept.reshape(walkers, ROWS, n).sum(axis=1)
    group = lax.broadcasted_iota(jnp.int32, (n, vectors), 0) // ROWS
    vector = lax.broadcasted_iota(jnp.int32, (n, vectors), 1)
    pick = (group == vector).astype(jnp.float32)
    out_ref[...] = jnp.dot(
        by_walker, pick, preferred_element_type=jnp.float32, precision=lax.Precision.HIGHEST
    )


def partial_bias(both, wdev):
    blocks, held, occupied, lanes = both.shape
    walkers, vectors = blocks * wdev, blocks * (held - wdev)
    return pl.pallas_call(
        functools.partial(bias_kernel, wdev),
        out_shape=jax.ShapeDtypeStruct((walkers, vectors), jnp.float32),
        in_specs=[pl.BlockSpec(memory_space=pltpu.VMEM)],
        out_specs=pl.BlockSpec(memory_space=pltpu.VMEM),
        cost_estimate=pl.CostEstimate(
            flops=2 * walkers * vectors * ROWS * occupied * lanes,
            bytes_accessed=2 * both.size,
            transcendentals=0,
        ),
        compiler_params=pltpu.CompilerParams(vmem_limit_bytes=16 * 1024 * 1024),
    )(both)


AROUND = (0, -1, 1, 2)
NEAR, NEXT = AROUND[:2], AROUND[2:]
HELD = ((NEAR, 0), (NEXT, 0), (NEAR, -1), (NEXT, -1), (NEAR, 1), (NEXT, 1), (NEAR, 2), (NEXT, 2))


EARLY = [(other, array) for other in (0, 1) for array in range(6)]
LATE = [(other, array) for other in (0, 1) for array in (6, 7)]


def assembly_kernel(which, *refs):
    blocks, (out_ref, sems) = refs[: len(which)], refs[-2:]
    height, width = blocks[0].shape[2:]
    x = lax.axis_index("walk_0") * 2 + lax.axis_index("blk_0")
    y, core = lax.axis_index("blk_1"), lax.axis_index("blk_2")
    copies = []
    for block, (other, array) in zip(blocks, which):
        colour = core if other == 0 else 1 - core
        kept, far = HELD[array]
        for k, near in enumerate(kept):
            dx = near + colour * (far - near)
            dy = far + colour * (near - far)
            bx, by = (x + dx + 4) % 4, (y + dy + 4) % 4
            for side in (0, 1):
                row = (((bx % 2) * 4 + by) * 2 + side) * 2 * height + (bx // 2) * height
                row = pl.multiple_of(row, height)
                column = pl.multiple_of(colour * width, width)
                copy = pltpu.make_async_copy(
                    block.at[k, side],
                    out_ref.at[pl.ds(row, height), pl.ds(column, width)],
                    sems.at[len(copies)],
                )
                copy.start()
                copies.append(copy)
    for copy in copies:
        copy.wait()


def assembled(which, blocks, orbitals, field=None):
    given = [] if field is None else [field]
    size = sum(block.size for block in blocks)
    return pl.pallas_call(
        functools.partial(assembly_kernel, which),
        out_shape=jax.ShapeDtypeStruct((orbitals, orbitals), jnp.bfloat16),
        in_specs=[pl.BlockSpec(memory_space=pl.ANY)] * len(blocks)
        + [pl.BlockSpec(memory_space=pltpu.VMEM)] * len(given),
        out_specs=pl.BlockSpec(memory_space=pltpu.VMEM),
        scratch_shapes=[pltpu.SemaphoreType.DMA((4 * len(blocks),))],
        input_output_aliases={len(blocks): 0} if given else {},
        cost_estimate=pl.CostEstimate(flops=size, bytes_accessed=4 * size, transcendentals=0),
        compiler_params=pltpu.CompilerParams(vmem_limit_bytes=24 * 1024 * 1024),
    )(*blocks, *given)


CHIP = ("blk_0", "blk_1", "blk_2", "walk_0")


def stepped(array, first, steps):
    def device(x, y, core):
        return (((x % 2) * 4 + y % 4) * 2 + core) * 2 + x % 4 // 2

    pairs = []
    for x in range(4):
        for y in range(4):
            for core in (0, 1):
                along_x = first == (core == 0)
                to = (x + steps, y) if along_x else (x, y + steps)
                pairs.append((device(x, y, core), device(*to, core)))
    return lax.ppermute(array, CHIP, pairs)


def other_core(array):
    return lax.ppermute(array, "blk_2", [(0, 1), (1, 0)])


def gathered(own):
    came = [own] + [stepped(own, True, -step) for step in AROUND[1:3]]
    came.append(stepped(own, True, AROUND[3]))
    near = jnp.stack(came[:2])
    below, above_near = stepped(near, False, 1), stepped(near, False, -1)
    next_ = jnp.stack(came[2:])
    above, below_next = stepped(next_, False, -1), stepped(next_, False, 1)
    far = [stepped(below, False, 1)]
    far.append(stepped(above, False, -1))
    mine = [near, next_, below, below_next, above_near, above] + far
    return [mine, [other_core(array) for array in mine]]


def copy_kernel(in_ref, out_ref):
    out_ref[...] = in_ref[...]


def copied(array):
    return pl.pallas_call(
        copy_kernel,
        out_shape=jax.ShapeDtypeStruct(array.shape, array.dtype),
        in_specs=[pl.BlockSpec(memory_space=pltpu.VMEM)],
        out_specs=pl.BlockSpec(memory_space=pltpu.VMEM),
        cost_estimate=pl.CostEstimate(
            flops=array.size, bytes_accessed=4 * array.size, transcendentals=0
        ),
        compiler_params=pltpu.CompilerParams(vmem_limit_bytes=4 * 1024 * 1024),
    )(array)


def column_blocks(array, count):
    *lead, columns = array.shape
    return jnp.moveaxis(array.reshape(*lead, count, columns // count), -2, 0)


def sum_kernel(scale_ref, *refs):
    raws, out_ref = refs[:-1], refs[-1]
    own, halves = raws[0].shape[:2]
    for h in range(halves):
        total = None
        for step, raw in enumerate(raws):
            for k in range(own):
                value = scale_ref[step * own + k] * raw[k, h].astype(jnp.float32)
                total = value if total is None else total + value
        out_ref[h] = total


def scaled_sum(scale, raws):
    own, *shape = raws[0].shape
    size = own * math.prod(shape) * len(raws)
    return pl.pallas_call(
        sum_kernel,
        out_shape=jax.ShapeDtypeStruct(tuple(shape), jnp.float32),
        in_specs=[pl.BlockSpec(memory_space=pltpu.SMEM)]
        + [pl.BlockSpec(memory_space=pltpu.VMEM)] * len(raws),
        out_specs=pl.BlockSpec(memory_space=pltpu.VMEM),
        cost_estimate=pl.CostEstimate(flops=2 * size, bytes_accessed=2 * size, transcendentals=0),
        compiler_params=pltpu.CompilerParams(vmem_limit_bytes=8 * 1024 * 1024),
    )(scale, *raws)


def at(array, index, dim):
    return lax.dynamic_index_in_dim(array, index, dim, keepdims=False, allow_negative_indices=False)


def exchanged(blocks, axes):
    return lax.all_to_all(blocks, axes, split_axis=0, concat_axis=0, tiled=True)


def part(walkers, inv_intersection, rotated_chol, full_chol, field_noise):
    wdev, double_rows, orbitals = walkers.shape
    occupied = double_rows // 2
    n_blk, n_walk = lax.axis_size(BLK), lax.axis_size(WALK)
    n_all = n_blk * n_walk

    inv = jnp.moveaxis(inv_intersection, 1, 2).reshape(wdev, occupied, double_rows)
    inv = jnp.pad(inv, ((0, 0), (0, -occupied % 8), (0, 0)))
    both = theta_and_chol(inv, walkers, rotated_chol, n_blk)
    both = exchanged(both, BLK)
    own = full_chol.shape[0]
    n_z = lax.axis_size("walk_1")
    half, at_z = lax.axis_index("walk_0"), lax.axis_index("walk_1")
    raw = full_chol.reshape(own, 2, n_z, -1, orbitals)

    def for_z(step):
        return at(raw, lax.rem(at_z + step, n_z), 2)

    slices = [for_z(step) for step in range(n_z)]
    raws = [copied(slices[0])]
    for step, rows in enumerate(slices[1:], 1):
        pairs = [(k, (k + step) % n_z) for k in range(n_z)]
        raws.append(lax.ppermute(rows, "walk_1", pairs))
    partial = partial_bias(both, wdev)
    vectors = partial.shape[1]

    summed = jnp.sum(partial, axis=0)
    rows = jnp.concatenate(
        [jnp.broadcast_to(summed, (n_blk, vectors)), partial.reshape(n_blk, wdev * vectors)], axis=1
    )
    rows = jnp.pad(rows, ((0, 0), (0, 128 - rows.shape[1])))
    rows = jnp.broadcast_to(rows[:, None, None], (n_blk, n_walk, 1, 128))
    core = lax.axis_index("blk_2")
    entry = lax.broadcasted_iota(jnp.int32, (n_z * own, vectors), 0)
    vector = lax.broadcasted_iota(jnp.int32, (n_z * own, vectors), 1)
    source = at_z - entry // own
    source = jnp.where(source < 0, source + n_z, source)
    wanted = (half * n_z + source) * own + entry % own
    ids = (half, at_z, core, vector == wanted)
    rows, (half, at_z, core, picked) = lax.optimization_barrier((rows, ids))
    rows = exchanged(rows.reshape(n_all, 1, 128), ALL)
    ids = (half, at_z, core, picked)
    rows, (half, at_z, core, picked) = lax.optimization_barrier((rows, ids))
    rows = rows.reshape(n_blk, n_walk, 128)
    bias_shift = jnp.sum(rows, axis=(0, 1))[:vectors] / math.sqrt(wdev * n_all)
    peers = at(rows, half * n_z + at_z, 1)
    bias = jnp.sum(peers, axis=0)[vectors : vectors + wdev * vectors].reshape(wdev, vectors)

    shifted = 0.1 * (field_noise - bias_shift)
    scale = jnp.sum(jnp.where(picked, shifted[None, :], 0.0), axis=1)
    part_field = scaled_sum(scale, raws)
    kept = at(part_field, half, 0)
    given = at(part_field, 1 - half, 0)
    came = lax.ppermute(given, "walk_0", [(0, 1), (1, 0)])
    came, bias = lax.optimization_barrier((came, bias))
    piece = (kept + came).astype(jnp.bfloat16)
    halves = column_blocks(piece, 2)[:, None]
    group = ("blk_2", "walk_1")
    halves = jnp.broadcast_to(halves, (2, n_z, *halves.shape[2:]))
    pieces = exchanged(halves.reshape(2 * n_z, *halves.shape[2:]), group)
    held = gathered(pieces.reshape(2, -1, orbitals // 2))
    field = assembled(EARLY, [held[other][array] for other, array in EARLY], orbitals)
    field = assembled(LATE, [held[other][array] for other, array in LATE], orbitals, field)
    current = walkers.reshape(wdev * double_rows, orbitals)
    total = current.astype(jnp.float32)
    for order in range(1, 5):
        current = (jnp.dot(current, field, preferred_element_type=jnp.float32) / order).astype(
            jnp.bfloat16
        )
        total = total + current.astype(jnp.float32)
    propagated = total.astype(jnp.bfloat16).reshape(walkers.shape)
    return propagated, bias, bias_shift


def solution(mesh):
    torus = Mesh(mesh.devices.reshape(2, 4, 2, 2, 8), ALL)
    in_specs = (
        P(ALL, None, None),
        P(ALL, None, None, None),
        P(BLK, None, None),
        P(WALK, BLK, None),
        P(),
    )
    out_specs = (P(ALL, None, None), P(ALL, None), P())
    return jax.shard_map(part, mesh=torus, in_specs=in_specs, out_specs=out_specs, check_vma=False)
```
